32 devices in a mesh: grp: 2 (over x), mem: 16 (over z, y, core).
Axes of the slice: x: 2, y: 2, z: 4, core: 2. Of those that a mesh axis runs over, the one named last changes fastest.
Arguments:
- phi_owned: float32 [8, 8, 8, 4096], P(None, None, None, ('grp', 'mem')), may hold values from -6 to 6
- band_counts: int32 [2, 16], P('grp'), may hold values from 1 to 128, 512 in all within a row
- neighbours: int32 [2, 6, 512], P('grp'), may hold values from -1 to 1023, as said below
Outputs:
- phi_new: float32 [8, 8, 8, 4096], P(None, None, None, ('grp', 'mem'))
The draws below stay inside these ranges and needn't reach their ends.
Inputs may be any that keep to these rules, and one draw needn't show every extreme that they name: `band_counts`: in every group the counts sum to 512, each is at least 1, and the largest is exactly 128. `neighbours`: tile k of a group lies at column k mod 16 and row k // 16 of the group's tile sheet. An entry is -1 (no neighbour) or the id of the tile across that face: tile k - 1, k + 1, k - 16, k + 16 of the same group for faces 0 to 3 (never across an edge of the sheet), tile k of group g - 1 or g + 1 for faces 4 and 5. Links are mutual.
All inputs are finite; a program needn't handle non-finite values.
Results may differ from the reference program's by a relative error of at most 0.0003.
Values sent between devices are 32-bit elements; how exact they have to be, the bound alone decides.
A program may use at most 64 MiB of HBM per device.

```python
import math
import jax
import jax.numpy as jnp
import numpy as np
from jax import lax

TILE = 8
STEPS = 4
HOLD_DEV = 32
OWN_DEV = 128
COLUMNS = 16
GROUPS = 2
GROUP_TILES = 512
SLOTS = 4096


def draw_neighbours(key, part):
    tile_count = GROUP_TILES
    tile_ids = jnp.arange(tile_count, dtype=jnp.int32)
    column = tile_ids % COLUMNS
    sheet_row = tile_ids // COLUMNS
    group_index = jnp.arange(GROUPS, dtype=jnp.int32)[:, None]
    subkeys = jax.random.split(jax.random.fold_in(key, 7), 3)
    link_x = jax.random.randint(subkeys[0], (GROUPS, tile_count), 0, 4) < 3
    link_y = jax.random.randint(subkeys[1], (GROUPS, tile_count), 0, 4) < 3
    link_z = jax.random.randint(subkeys[2], (GROUPS, tile_count), 0, 4) < 3
    group_base = group_index * tile_count
    present = [(column > 0) & jnp.roll(link_x, 1, axis=1), (column < COLUMNS - 1) & link_x, (sheet_row > 0) & jnp.roll(link_y, COLUMNS, axis=1), (sheet_row < HOLD_DEV - 1) & link_y, (group_index > 0) & jnp.roll(link_z, 1, axis=0), (group_index < GROUPS - 1) & link_z]
    targets = [group_base + tile_ids - 1, group_base + tile_ids + 1, group_base + tile_ids - COLUMNS, group_base + tile_ids + COLUMNS, group_base - tile_count + tile_ids, group_base + tile_count + tile_ids]
    stacked = [jnp.where(linked, target, -1) for linked, target in zip(present, targets)]
    return jnp.stack(stacked, axis=1).astype(jnp.int32)


def block_scale(key, dims, cuts, smallest, high):
    level = 1.0
    for position, shards_of in cuts:
        heights = jax.random.uniform(jax.random.fold_in(jax.random.fold_in(key, 6), position), (shards_of,), jnp.float32, smallest / len(cuts), high / len(cuts))
        level = level * jnp.repeat(jnp.exp(heights), dims[position] // shards_of).reshape((-1,) + (1,) * (len(dims) - 1 - position))
    return level


def length_profile(amount, total, limit, lean):
    weights = [(1 << 20) // math.isqrt(grade ** lean) + 1 for grade in range(2, amount + 1)]
    spare, holding = total - limit - (amount - 1), [1] * (amount - 1)
    while spare > 0:
        movable = [i for i in range(amount - 1) if holding[i] < limit]
        mass, budget = sum([weights[i] for i in movable]), spare
        for i in movable:
            addition = min(limit - holding[i], max(1, budget * weights[i] // mass), spare)
            holding[i] = holding[i] + addition
            spare = spare - addition
    return np.array([limit] + holding)


def ragged_sizes(key, amount, total, bound, slope):
    if amount == 2:
        one = jax.random.randint(key, (), max(1, total - bound), min(bound, total - 1) + 1)
        return jnp.stack([one, total - one])
    sizes = jnp.asarray(length_profile(amount, total, bound, slope), jnp.int32)
    pairs = (amount - 1) // 2
    giver, sink = sizes[1:1 + 2 * pairs:2], sizes[2:2 + 2 * pairs:2]
    slack = jnp.minimum(giver - 1, bound - sink)
    passed = jax.random.randint(jax.random.fold_in(key, 1), (pairs,), 0, 1 << 20) % (slack + 1)
    sizes = sizes.at[1:1 + 2 * pairs:2].set(giver - passed).at[2:2 + 2 * pairs:2].set(sink + passed)
    return sizes[jax.random.permutation(jax.random.fold_in(key, 2), amount)]


def gaussian(rng, dims, spread, limit, shards=(), kind=jnp.bfloat16):
    values = jax.random.normal(rng, dims, jnp.float32) * spread
    if len(shards) > 0:
        values = block_scale(rng, dims, shards, -0.22, 0.18) * values
    return jnp.clip(values, min=-limit, max=limit).astype(kind)


def setup_inputs(seed: int = 0) -> dict:
    arg_keys = jax.random.split(jax.random.key(seed), 4)
    phi_owned = gaussian(arg_keys[0], (TILE, TILE, TILE, SLOTS), 1.0, 6.0, ((3, 32),), jnp.float32)
    band_counts = jax.vmap(lambda own: ragged_sizes(own, COLUMNS, GROUP_TILES, OWN_DEV, 2))(jax.random.split(arg_keys[1], GROUPS)).reshape((GROUPS, COLUMNS)).astype(jnp.int32)
    neighbours = draw_neighbours(jax.random.fold_in(arg_keys[3], 71), 0)
    return {"phi_owned": phi_owned, "band_counts": band_counts, "neighbours": neighbours}


TIME_STEP = 0.5
EPSILON = 1e-06

def upwind(backward, forward, positive):
    rising = jnp.maximum(jnp.square(jnp.maximum(backward, 0.0)), jnp.square(jnp.minimum(forward, 0.0)))
    falling = jnp.maximum(jnp.square(jnp.minimum(backward, 0.0)), jnp.square(jnp.maximum(forward, 0.0)))
    return jnp.where(positive, rising, falling)

def reference(phi_owned, band_counts, neighbours):
    tile_edge = phi_owned.shape[0]
    groups, columns = band_counts.shape
    tile_total = neighbours.shape[2]
    own_slots = phi_owned.shape[3] // (groups * columns)
    counts = band_counts.astype(jnp.int32)
    starts = (jnp.cumsum(counts, axis=1) - counts).astype(jnp.int32)
    tile_ids = jnp.arange(tile_total, dtype=jnp.int32)
    owner_mask = (starts[:, None, :] <= tile_ids[None, :, None]).astype(jnp.int32)
    owner_of = (lax.optimization_barrier(jnp.sum(owner_mask, axis=2)) - 1).astype(jnp.int32)
    first_tile = jnp.take_along_axis(starts, owner_of, axis=1).astype(jnp.int32)
    group_ids = jnp.arange(groups, dtype=jnp.int32)[:, None]
    slot_index = ((group_ids * columns + owner_of) * own_slots + tile_ids[None, :] - first_tile).reshape(-1).astype(jnp.int32)
    level_set = jnp.take(phi_owned, slot_index, axis=3)
    sign_field = level_set / jnp.sqrt(level_set * level_set + 1.0)
    positive = sign_field > 0
    link_table = jnp.transpose(neighbours, (1, 0, 2)).reshape(6, groups * tile_total)
    present = link_table >= 0
    safe_ids = jnp.maximum(link_table, 0).astype(jnp.int32)
    for sweep in range(STEPS):
        squares = jnp.zeros_like(level_set)
        for direction in range(3):
            low_layer = lax.index_in_dim(level_set, 0, direction, keepdims=True)
            high_layer = lax.index_in_dim(level_set, tile_edge - 1, direction, keepdims=True)
            below = jnp.where(present[2 * direction], jnp.take(high_layer, safe_ids[2 * direction], axis=3), low_layer)
            above = jnp.where(present[2 * direction + 1], jnp.take(low_layer, safe_ids[2 * direction + 1], axis=3), high_layer)
            extended = jnp.concatenate([below, level_set, above], axis=direction)
            backward = level_set - lax.slice_in_dim(extended, 0, tile_edge, axis=direction)
            forward = lax.slice_in_dim(extended, 2, tile_edge + 2, axis=direction) - level_set
            squares = squares + upwind(backward, forward, positive)
        level_set = level_set - TIME_STEP * sign_field * (jnp.sqrt(squares + EPSILON) - 1.0)
    return jnp.zeros_like(phi_owned).at[:, :, :, slot_index].set(level_set)
```

```python
import functools

import jax
import jax.numpy as jnp
from jax import lax
from jax.experimental import pallas as pl
from jax.experimental.pallas import tpu as pltpu
from jax.sharding import PartitionSpec as P

STEPS = 4
TIME_STEP = 0.5
EPSILON = 1e-06
LANES = 128
F32 = jnp.float32


def roll(x, shift, axis):
    shift = shift % x.shape[axis]
    return x if shift == 0 else pltpu.roll(x, shift, axis)


def dot(a, b, dims):
    return lax.dot_general(
        a, b, (dims, ((), ())), precision=lax.Precision.HIGHEST, preferred_element_type=F32
    )


def kernel(
    columns, groups, phi_ref, place_ref, live_ref, arrive_ref, depart_ref, links_ref, out_ref,
    leave, land, back, home, up, down, from_below, from_above, right, left, from_left, from_right,
    level, sign, out_send, out_recv, back_send, back_recv, side_send, side_recv,
):
    edge = phi_ref.shape[0]
    rows = arrive_ref.shape[0]
    halo = STEPS
    wide = 2 * edge
    layers = edge + 2 * halo
    me, grp = lax.axis_index("mem"), lax.axis_index("grp")
    has_left, has_right = me > 0, me < columns - 1
    has_below, has_above = grp > 0, grp < groups - 1

    for ref in (from_below, from_above, from_left, from_right):
        ref[...] = jnp.zeros_like(ref)

    barrier = pltpu.get_barrier_semaphore()
    for d in range(1, columns):
        pl.semaphore_signal(barrier, inc=1, device_id={"mem": lax.rem(me + d, columns)},
                            device_id_type=pl.DeviceIdType.MESH)

    @pl.when(has_below)
    def _():
        pl.semaphore_signal(barrier, inc=1, device_id={"grp": grp - 1},
                            device_id_type=pl.DeviceIdType.MESH)

    @pl.when(has_above)
    def _():
        pl.semaphore_signal(barrier, inc=1, device_id={"grp": grp + 1},
                            device_id_type=pl.DeviceIdType.MESH)

    def exchange(source, target, send, recv):
        started = []
        for d in range(1, columns):
            peer = lax.rem(me + d, columns)
            copy = pltpu.make_async_remote_copy(
                src_ref=source.at[peer], dst_ref=target.at[me],
                send_sem=send.at[d], recv_sem=recv.at[d],
                device_id={"mem": peer}, device_id_type=pl.DeviceIdType.MESH)
            copy.start()
            started.append(copy)
        target[me] = source[me]
        for d in range(1, columns):
            origin = lax.rem(me + columns - d, columns)
            pltpu.make_async_remote_copy(
                src_ref=source.at[origin], dst_ref=target.at[origin],
                send_sem=send.at[d], recv_sem=recv.at[d],
                device_id={"mem": origin}, device_id_type=pl.DeviceIdType.MESH).wait_recv()
        return started

    def shift_copy(source, target, index, axis, peer):
        return pltpu.make_async_remote_copy(
            src_ref=source, dst_ref=target, send_sem=side_send.at[index],
            recv_sem=side_recv.at[index], device_id={axis: peer},
            device_id_type=pl.DeviceIdType.MESH)

    def both_ways(axis, here, more, less, ahead, behind, target_of_ahead, target_of_behind, base):
        to_ahead = shift_copy(ahead, target_of_ahead, base, axis, here + 1)
        to_behind = shift_copy(behind, target_of_behind, base + 1, axis, here - 1)
        pl.when(more)(to_ahead.start)
        pl.when(less)(to_behind.start)
        pl.when(less)(to_ahead.wait_recv)
        pl.when(more)(to_behind.wait_recv)
        pl.when(more)(to_ahead.wait_send)
        pl.when(less)(to_behind.wait_send)

    cells = jnp.concatenate(
        [phi_ref[2 * pair + k, y] for pair in range(edge // 2) for y in range(edge) for k in range(2)],
        axis=0)
    leave[...] = dot(place_ref[...], cells, ((1,), (1,))).reshape(leave.shape)

    tiles = links_ref.shape[1]
    chosen = (lax.broadcasted_iota(jnp.int32, (rows, tiles), 0) * columns + me
              == lax.broadcasted_iota(jnp.int32, (rows, tiles), 1))

    def link(face):
        there = jnp.where(links_ref[face:face + 1, :] >= 0, 1.0, 0.0).astype(F32)
        value = jnp.sum(jnp.where(chosen, there, 0.0), axis=1, keepdims=True)
        return jnp.broadcast_to(value, (rows, LANES))

    link_x = [link(0), link(1)]
    link_y = link(2)
    link_z = [link(4), link(5)]
    lane = lax.broadcasted_iota(jnp.int32, (rows, LANES), 1)
    z = lane % wide

    pl.semaphore_wait(barrier, columns - 1 + has_below.astype(jnp.int32) + has_above.astype(jnp.int32))
    sent = exchange(leave, land, out_send, out_recv)

    packed = dot(arrive_ref[...], land[...].reshape(-1, land.shape[2]), ((1,), (0,)))
    mine = []
    for pair in range(edge // 2):
        both = packed[:, pair * LANES:(pair + 1) * LANES]
        mine += [roll(both, halo, 1), roll(both, halo - edge, 1)]

    parts = mine + [link_y] + link_x
    slots = up.shape[0]
    for q in range(slots):
        high, low = jnp.zeros((rows, LANES), F32), jnp.zeros((rows, LANES), F32)
        for k in range(4):
            if 4 * q + k < len(parts):
                inside = (z >= halo * k) & (z < halo * (k + 1))
                part = parts[4 * q + k]
                high = jnp.where(inside, roll(part, halo * k - edge, 1), high)
                low = jnp.where(inside, roll(part, halo * k - halo, 1), low)
        up[q] = high
        down[q] = low
    both_ways("grp", grp, has_above, has_below, up, down, from_below, from_above, 0)

    filled = []
    for i, part in enumerate(parts):
        q, k = divmod(i, 4)
        below = roll(from_below[q], -halo * k, 1)
        above = roll(from_above[q], halo + edge - halo * k, 1)
        filled.append(jnp.where(z < halo, below, jnp.where(z >= halo + edge, above, part)))
    mine, link_y, link_x = filled[:edge], filled[edge], filled[edge + 1:]
    link_z = jnp.where(z == halo, link_z[0], jnp.where(z == halo + edge, link_z[1],
                       jnp.where(z == 0, 0.0, 1.0)))
    link_y = jnp.where(lane < wide, link_y, 1.0)

    for k in range(halo):
        right[k] = mine[edge - halo + k]
        left[k] = mine[k]
    for ref in (right, left):
        ref[halo] = link_y
        ref[halo + 1] = link_z
    both_ways("mem", me, has_right, has_left, right, left, from_left, from_right, 2)

    masks_y = [from_left[halo], link_y, from_right[halo]]
    masks_z = [from_left[halo + 1], link_z, from_right[halo + 1]]
    for i in range(layers):
        if i < halo:
            value = from_left[i]
        elif i < halo + edge:
            value = mine[i - halo]
        else:
            value = from_right[i - halo - edge]
        level[0, i] = value
        sign[i] = value / jnp.sqrt(value * value + 1.0)

    for step in range(STEPS):
        now, later = step % 2, (step + 1) % 2
        gap = None
        for i in range(step + 1, layers - 1 - step):
            region = 0 if i < halo else (1 if i < halo + edge else 2)
            mask_y, mask_z = masks_y[region], masks_z[region]
            value, field = level[now, i], sign[i]
            side = jnp.where(field > 0, 1.0, -1.0)

            def across(j):
                change = level[now, j] - level[now, j - 1]
                if j == halo:
                    change = change * link_x[0]
                elif j == halo + edge:
                    change = change * link_x[1]
                return change

            gap = across(i) if gap is None else gap
            ahead = across(i + 1)
            most = jnp.maximum(jnp.maximum(side * gap, -(side * ahead)), 0.0)
            squares = most * most
            gap = ahead

            turned = roll(value, wide, 1)
            before = jnp.where(lane < wide, roll(turned, 1, 0), turned)
            behind = (value - before) * mask_y
            turned = roll(behind, -wide, 1)
            ahead = jnp.where(lane >= LANES - wide, roll(turned, -1, 0), turned)
            most = jnp.maximum(jnp.maximum(side * behind, -(side * ahead)), 0.0)
            squares = squares + most * most

            behind = (value - roll(value, 1, 1)) * mask_z
            ahead = roll(behind, -1, 1)
            most = jnp.maximum(jnp.maximum(side * behind, -(side * ahead)), 0.0)
            squares = squares + most * most
            level[later, i] = value - TIME_STEP * field * (jnp.sqrt(squares + EPSILON) - 1.0)

    last = STEPS % 2
    pairs = []
    for pair in range(edge // 2):
        first, second = level[last, halo + 2 * pair], level[last, halo + 2 * pair + 1]
        pairs.append(jnp.where(z < edge, roll(first, -halo, 1), roll(second, edge - halo, 1)))
    final = jnp.concatenate(pairs, axis=1)
    back[...] = dot(depart_ref[...], final, ((1,), (0,))).reshape(back.shape)
    sent += exchange(back, home, back_send, back_recv)

    owned = dot(live_ref[...], home[...].reshape(-1, home.shape[2]), ((1,), (0,))).T
    for pair in range(edge // 2):
        for y in range(edge):
            for k in range(2):
                at = ((pair * edge + y) * 2 + k) * edge
                out_ref[2 * pair + k, y] = owned[at:at + edge]
    for copy in sent:
        copy.wait_send()


def on_device(phi_owned, band_counts, neighbours):
    edge, own_slots = phi_owned.shape[0], phi_owned.shape[3]
    columns, groups = lax.axis_size("mem"), lax.axis_size("grp")
    me = lax.axis_index("mem")
    rows = neighbours.shape[2] // columns
    depth = -(-own_slots // columns)
    padded = -(-depth // 8) * 8
    counts = band_counts[0]
    owners = jnp.arange(columns, dtype=jnp.int32)
    first = jnp.sum(jnp.where(owners < me, counts, 0))
    count = jnp.sum(jnp.where(owners == me, counts, 0))
    slot = jnp.arange(own_slots, dtype=jnp.int32)[None, :]
    entry = jnp.arange(columns * padded, dtype=jnp.int32)
    block, place = entry // padded, entry % padded
    chosen = ((first + slot) % columns == block[:, None]) & (slot // columns == place[:, None])
    placing = chosen.astype(F32)
    living = (chosen & (slot < count)).astype(F32).T
    starts = jnp.sum(jnp.where(owners[:, None] < block[None, :], counts[:, None], 0), axis=0)
    lengths = jnp.sum(jnp.where(owners[:, None] == block[None, :], counts[:, None], 0), axis=0)
    offset = (jnp.arange(rows, dtype=jnp.int32) * columns + me)[:, None] - starts[None, :]
    arrive = ((offset >= 0) & (offset < lengths[None, :])
              & (jnp.maximum(offset, 0) // columns == place[None, :])).astype(F32)
    halo, cells = STEPS, edge * edge * edge
    vmem = pl.BlockSpec(memory_space=pltpu.VMEM)
    buffer = pltpu.VMEM((columns, padded, cells), F32)
    strip = pltpu.VMEM((-(-(edge + 3) // 4), rows, LANES), F32)
    face = pltpu.VMEM((halo + 2, rows, LANES), F32)
    layers = edge + 2 * halo
    return pl.pallas_call(
        functools.partial(kernel, columns, groups),
        out_shape=jax.ShapeDtypeStruct(phi_owned.shape, F32),
        in_specs=[vmem] * 6,
        out_specs=vmem,
        scratch_shapes=[buffer] * 4 + [strip] * 4 + [face] * 4 + [
            pltpu.VMEM((2, layers, rows, LANES), F32),
            pltpu.VMEM((layers, rows, LANES), F32),
        ] + [pltpu.SemaphoreType.DMA((columns,))] * 4 + [pltpu.SemaphoreType.DMA((4,))] * 2,
        compiler_params=pltpu.CompilerParams(collective_id=0, has_side_effects=True),
    )(phi_owned, placing, living, arrive, arrive.T, neighbours[0])


def solution(mesh):
    return jax.shard_map(
        on_device,
        mesh=mesh,
        in_specs=(P(None, None, None, ("grp", "mem")), P("grp", None), P("grp", None, None)),
        out_specs=P(None, None, None, ("grp", "mem")),
        check_vma=False,
    )
```

```python
import functools

import jax
import jax.numpy as jnp
from jax import lax
from jax.experimental import pallas as pl
from jax.experimental.pallas import tpu as pltpu
from jax.sharding import PartitionSpec as P

STEPS = 4
TIME_STEP = 0.5
EPSILON = 1e-06
LANES = 128
F32 = jnp.float32


def roll(x, shift, axis):
    shift = shift % x.shape[axis]
    return x if shift == 0 else pltpu.roll(x, shift, axis)


def dot(a, b, dims):
    return lax.dot_general(
        a, b, (dims, ((), ())), precision=lax.Precision.HIGHEST, preferred_element_type=F32
    )


def kernel(
    columns, groups, phi_ref, counts_ref, links_ref, out_ref,
    leave, land, back, home, up, down, from_below, from_above, right, left, from_left, from_right,
    level, sign, out_send, out_recv, back_send, back_recv, side_send, side_recv,
):
    edge = phi_ref.shape[0]
    own_slots = phi_ref.shape[3]
    padded, tiles = leave.shape[1], links_ref.shape[2]
    rows = tiles // columns
    halo = STEPS
    wide = 2 * edge
    layers = edge + 2 * halo
    me, grp = lax.axis_index("mem"), lax.axis_index("grp")
    has_left, has_right = me > 0, me < columns - 1
    has_below, has_above = grp > 0, grp < groups - 1

    for ref in (from_below, from_above, from_left, from_right):
        ref[...] = jnp.zeros_like(ref)

    barrier = pltpu.get_barrier_semaphore()
    for d in range(1, columns):
        pl.semaphore_signal(barrier, inc=1, device_id={"mem": lax.rem(me + d, columns)},
                            device_id_type=pl.DeviceIdType.MESH)

    @pl.when(has_below)
    def _():
        pl.semaphore_signal(barrier, inc=1, device_id={"grp": grp - 1},
                            device_id_type=pl.DeviceIdType.MESH)

    @pl.when(has_above)
    def _():
        pl.semaphore_signal(barrier, inc=1, device_id={"grp": grp + 1},
                            device_id_type=pl.DeviceIdType.MESH)

    def exchange(source, target, send, recv):
        started = []
        for d in range(1, columns):
            peer = lax.rem(me + d, columns)
            copy = pltpu.make_async_remote_copy(
                src_ref=source.at[peer], dst_ref=target.at[me],
                send_sem=send.at[d], recv_sem=recv.at[d],
                device_id={"mem": peer}, device_id_type=pl.DeviceIdType.MESH)
            copy.start()
            started.append(copy)
        target[me] = source[me]
        for d in range(1, columns):
            origin = lax.rem(me + columns - d, columns)
            pltpu.make_async_remote_copy(
                src_ref=source.at[origin], dst_ref=target.at[origin],
                send_sem=send.at[d], recv_sem=recv.at[d],
                device_id={"mem": origin}, device_id_type=pl.DeviceIdType.MESH).wait_recv()
        return started

    def shift_copy(source, target, index, axis, peer):
        return pltpu.make_async_remote_copy(
            src_ref=source, dst_ref=target, send_sem=side_send.at[index],
            recv_sem=side_recv.at[index], device_id={axis: peer},
            device_id_type=pl.DeviceIdType.MESH)

    def both_ways(axis, here, more, less, ahead, behind, target_of_ahead, target_of_behind, base):
        to_ahead = shift_copy(ahead, target_of_ahead, base, axis, here + 1)
        to_behind = shift_copy(behind, target_of_behind, base + 1, axis, here - 1)
        pl.when(more)(to_ahead.start)
        pl.when(less)(to_behind.start)
        pl.when(less)(to_ahead.wait_recv)
        pl.when(more)(to_behind.wait_recv)
        pl.when(more)(to_ahead.wait_send)
        pl.when(less)(to_behind.wait_send)

    count_of = [counts_ref[0, m] for m in range(columns)]
    first, count = jnp.int32(0), jnp.int32(0)
    for m in range(columns):
        first = first + jnp.where(m < me, count_of[m], 0)
        count = count + jnp.where(m == me, count_of[m], 0)
    entries = columns * padded
    slot = lax.broadcasted_iota(jnp.int32, (1, own_slots), 1)
    key = (first + slot) % columns * padded + slot // columns
    chosen = lax.broadcasted_iota(jnp.int32, (entries, own_slots), 0) == key
    placing = jnp.where(chosen, 1.0, 0.0).astype(F32)
    entry = lax.broadcasted_iota(jnp.int32, (1, entries), 1)
    block, place = entry // padded, entry % padded
    start, length = jnp.zeros((1, entries), jnp.int32), jnp.zeros((1, entries), jnp.int32)
    for m in range(columns):
        start = start + jnp.where(block > m, count_of[m], 0)
        length = length + jnp.where(block == m, count_of[m], 0)
    offset = lax.broadcasted_iota(jnp.int32, (rows, entries), 0) * columns + me - start
    begin = place * columns
    arrive = jnp.where((offset >= begin) & (offset < begin + columns) & (offset < length),
                       1.0, 0.0).astype(F32)

    cells = jnp.concatenate(
        [phi_ref[2 * pair + k, y] for pair in range(edge // 2) for y in range(edge) for k in range(2)],
        axis=0)
    leave[...] = dot(placing, cells, ((1,), (1,))).reshape(leave.shape)

    held = (lax.broadcasted_iota(jnp.int32, (rows, tiles), 0) * columns + me
            == lax.broadcasted_iota(jnp.int32, (rows, tiles), 1))

    def link(face):
        there = jnp.where(links_ref[face] >= 0, 1.0, 0.0).astype(F32)
        value = jnp.sum(jnp.where(held, there, 0.0), axis=1, keepdims=True)
        return jnp.broadcast_to(value, (rows, LANES))

    link_x = [link(0), link(1)]
    link_y = link(2)
    link_z = [link(4), link(5)]
    lane = lax.broadcasted_iota(jnp.int32, (rows, LANES), 1)
    z = lane % wide

    pl.semaphore_wait(barrier, columns - 1 + has_below.astype(jnp.int32) + has_above.astype(jnp.int32))
    sent = exchange(leave, land, out_send, out_recv)

    packed = dot(arrive, land[...].reshape(-1, land.shape[2]), ((1,), (0,)))
    mine = []
    for pair in range(edge // 2):
        both = packed[:, pair * LANES:(pair + 1) * LANES]
        mine += [roll(both, halo, 1), roll(both, halo - edge, 1)]

    parts = mine + [link_y] + link_x
    slots = up.shape[0]
    for q in range(slots):
        high, low = jnp.zeros((rows, LANES), F32), jnp.zeros((rows, LANES), F32)
        for k in range(4):
            if 4 * q + k < len(parts):
                inside = (z >= halo * k) & (z < halo * (k + 1))
                part = parts[4 * q + k]
                high = jnp.where(inside, roll(part, halo * k - edge, 1), high)
                low = jnp.where(inside, roll(part, halo * k - halo, 1), low)
        up[q] = high
        down[q] = low
    both_ways("grp", grp, has_above, has_below, up, down, from_below, from_above, 0)

    filled = []
    for i, part in enumerate(parts):
        q, k = divmod(i, 4)
        below = roll(from_below[q], -halo * k, 1)
        above = roll(from_above[q], halo + edge - halo * k, 1)
        filled.append(jnp.where(z < halo, below, jnp.where(z >= halo + edge, above, part)))
    mine, link_y, link_x = filled[:edge], filled[edge], filled[edge + 1:]
    link_z = jnp.where(z == halo, link_z[0], jnp.where(z == halo + edge, link_z[1],
                       jnp.where(z == 0, 0.0, 1.0)))
    link_y = jnp.where(lane < wide, link_y, 1.0)

    for k in range(halo):
        right[k] = mine[edge - halo + k]
        left[k] = mine[k]
    for ref in (right, left):
        ref[halo] = link_y
        ref[halo + 1] = link_z
    both_ways("mem", me, has_right, has_left, right, left, from_left, from_right, 2)

    masks_y = [from_left[halo], link_y, from_right[halo]]
    masks_z = [from_left[halo + 1], link_z, from_right[halo + 1]]
    for i in range(layers):
        if i < halo:
            value = from_left[i]
        elif i < halo + edge:
            value = mine[i - halo]
        else:
            value = from_right[i - halo - edge]
        level[0, i] = value
        sign[i] = value / jnp.sqrt(value * value + 1.0)

    for step in range(STEPS):
        now, later = step % 2, (step + 1) % 2
        gap = None
        for i in range(step + 1, layers - 1 - step):
            region = 0 if i < halo else (1 if i < halo + edge else 2)
            mask_y, mask_z = masks_y[region], masks_z[region]
            value, field = level[now, i], sign[i]
            side = jnp.where(field > 0, 1.0, -1.0)

            def across(j):
                change = level[now, j] - level[now, j - 1]
                if j == halo:
                    change = change * link_x[0]
                elif j == halo + edge:
                    change = change * link_x[1]
                return change

            gap = across(i) if gap is None else gap
            ahead = across(i + 1)
            most = jnp.maximum(jnp.maximum(side * gap, -(side * ahead)), 0.0)
            squares = most * most
            gap = ahead

            turned = roll(value, wide, 1)
            before = jnp.where(lane < wide, roll(turned, 1, 0), turned)
            behind = (value - before) * mask_y
            turned = roll(behind, -wide, 1)
            ahead = jnp.where(lane >= LANES - wide, roll(turned, -1, 0), turned)
            most = jnp.maximum(jnp.maximum(side * behind, -(side * ahead)), 0.0)
            squares = squares + most * most

            behind = (value - roll(value, 1, 1)) * mask_z
            ahead = roll(behind, -1, 1)
            most = jnp.maximum(jnp.maximum(side * behind, -(side * ahead)), 0.0)
            squares = squares + most * most
            level[later, i] = value - TIME_STEP * field * (jnp.sqrt(squares + EPSILON) - 1.0)

    last = STEPS % 2
    pairs = []
    for pair in range(edge // 2):
        first, second = level[last, halo + 2 * pair], level[last, halo + 2 * pair + 1]
        pairs.append(jnp.where(z < edge, roll(first, -halo, 1), roll(second, edge - halo, 1)))
    final = jnp.concatenate(pairs, axis=1)
    back[...] = dot(arrive, final, ((0,), (0,))).reshape(back.shape)
    sent += exchange(back, home, back_send, back_recv)

    living = jnp.where(slot < count, placing, 0.0)
    owned = dot(living, home[...].reshape(-1, home.shape[2]), ((0,), (0,))).T
    for pair in range(edge // 2):
        for y in range(edge):
            for k in range(2):
                at = ((pair * edge + y) * 2 + k) * edge
                out_ref[2 * pair + k, y] = owned[at:at + edge]
    for copy in sent:
        copy.wait_send()


def on_device(phi_owned, band_counts, neighbours):
    edge, own_slots = phi_owned.shape[0], phi_owned.shape[3]
    columns, groups = lax.axis_size("mem"), lax.axis_size("grp")
    rows = neighbours.shape[2] // columns
    padded = -(-own_slots // (8 * columns)) * 8
    halo, cells = STEPS, edge * edge * edge
    vmem = pl.BlockSpec(memory_space=pltpu.VMEM)
    buffer = pltpu.VMEM((columns, padded, cells), F32)
    strip = pltpu.VMEM((-(-(edge + 3) // 4), rows, LANES), F32)
    face = pltpu.VMEM((halo + 2, rows, LANES), F32)
    layers = edge + 2 * halo
    return pl.pallas_call(
        functools.partial(kernel, columns, groups),
        out_shape=jax.ShapeDtypeStruct(phi_owned.shape, F32),
        in_specs=[vmem, pl.BlockSpec(memory_space=pltpu.SMEM), vmem],
        out_specs=vmem,
        scratch_shapes=[buffer] * 4 + [strip] * 4 + [face] * 4 + [
            pltpu.VMEM((2, layers, rows, LANES), F32),
            pltpu.VMEM((layers, rows, LANES), F32),
        ] + [pltpu.SemaphoreType.DMA((columns,))] * 4 + [pltpu.SemaphoreType.DMA((4,))] * 2,
        compiler_params=pltpu.CompilerParams(collective_id=0, has_side_effects=True),
    )(phi_owned, band_counts, jnp.transpose(neighbours, (1, 0, 2)))


def solution(mesh):
    return jax.shard_map(
        on_device,
        mesh=mesh,
        in_specs=(P(None, None, None, ("grp", "mem")), P("grp", None), P("grp", None, None)),
        out_specs=P(None, None, None, ("grp", "mem")),
        check_vma=False,
    )
```

```python
import functools

import jax
import jax.numpy as jnp
from jax import lax
from jax.experimental import pallas as pl
from jax.experimental.pallas import tpu as pltpu
from jax.sharding import PartitionSpec as P

STEPS = 4
TIME_STEP = 0.5
EPSILON = 1e-06
LANES = 128
F32 = jnp.float32


def roll(x, shift, axis):
    shift = shift % x.shape[axis]
    return x if shift == 0 else pltpu.roll(x, shift, axis)


def dot(a, b, dims):
    return lax.dot_general(
        a, b, (dims, ((), ())), precision=lax.Precision.HIGHEST, preferred_element_type=F32
    )


def kernel(
    columns, groups, phi_ref, counts_ref, links_ref, out_ref,
    leave, land, back, home, up, down, from_below, from_above, right, left, from_left, from_right,
    level, sign, out_send, out_recv, back_send, back_recv, side_send, side_recv,
):
    edge = phi_ref.shape[0]
    own_slots = phi_ref.shape[3]
    padded, tiles = leave.shape[1], links_ref.shape[2]
    rows = tiles // columns
    halo = STEPS
    wide = 2 * edge
    layers = edge + 2 * halo
    me, grp = lax.axis_index("mem"), lax.axis_index("grp")
    has_left, has_right = me > 0, me < columns - 1
    has_below, has_above = grp > 0, grp < groups - 1

    for ref in (from_below, from_above, from_left, from_right):
        ref[...] = jnp.zeros_like(ref)

    barrier = pltpu.get_barrier_semaphore()
    for d in range(1, columns):
        pl.semaphore_signal(barrier, inc=1, device_id={"mem": lax.rem(me + d, columns)},
                            device_id_type=pl.DeviceIdType.MESH)

    @pl.when(has_below)
    def _():
        pl.semaphore_signal(barrier, inc=1, device_id={"grp": grp - 1},
                            device_id_type=pl.DeviceIdType.MESH)

    @pl.when(has_above)
    def _():
        pl.semaphore_signal(barrier, inc=1, device_id={"grp": grp + 1},
                            device_id_type=pl.DeviceIdType.MESH)

    def exchange(source, target, send, recv):
        started = []
        for d in range(1, columns):
            peer = lax.rem(me + d, columns)
            copy = pltpu.make_async_remote_copy(
                src_ref=source.at[peer], dst_ref=target.at[me],
                send_sem=send.at[d], recv_sem=recv.at[d],
                device_id={"mem": peer}, device_id_type=pl.DeviceIdType.MESH)
            copy.start()
            started.append(copy)
        target[me] = source[me]
        for d in range(1, columns):
            origin = lax.rem(me + columns - d, columns)
            pltpu.make_async_remote_copy(
                src_ref=source.at[origin], dst_ref=target.at[origin],
                send_sem=send.at[d], recv_sem=recv.at[d],
                device_id={"mem": origin}, device_id_type=pl.DeviceIdType.MESH).wait_recv()
        return started

    def shift_copy(source, target, index, axis, peer):
        return pltpu.make_async_remote_copy(
            src_ref=source, dst_ref=target, send_sem=side_send.at[index],
            recv_sem=side_recv.at[index], device_id={axis: peer},
            device_id_type=pl.DeviceIdType.MESH)

    def both_ways(axis, here, more, less, ahead, behind, target_of_ahead, target_of_behind, base):
        to_ahead = shift_copy(ahead, target_of_ahead, base, axis, here + 1)
        to_behind = shift_copy(behind, target_of_behind, base + 1, axis, here - 1)
        pl.when(more)(to_ahead.start)
        pl.when(less)(to_behind.start)
        late.extend([(more, to_ahead), (less, to_behind)])

        def arrived():
            pl.when(less)(to_ahead.wait_recv)
            pl.when(more)(to_behind.wait_recv)

        return arrived

    late = []

    count_of = [counts_ref[0, m] for m in range(columns)]
    first, count = jnp.int32(0), jnp.int32(0)
    for m in range(columns):
        first = first + jnp.where(m < me, count_of[m], 0)
        count = count + jnp.where(m == me, count_of[m], 0)
    entries = columns * padded
    slot = lax.broadcasted_iota(jnp.int32, (1, own_slots), 1)
    key = (first + slot) % columns * padded + slot // columns
    chosen = lax.broadcasted_iota(jnp.int32, (entries, own_slots), 0) == key
    placing = jnp.where(chosen, 1.0, 0.0).astype(F32)
    entry = lax.broadcasted_iota(jnp.int32, (1, entries), 1)
    block, place = entry // padded, entry % padded
    start, length = jnp.zeros((1, entries), jnp.int32), jnp.zeros((1, entries), jnp.int32)
    for m in range(columns):
        start = start + jnp.where(block > m, count_of[m], 0)
        length = length + jnp.where(block == m, count_of[m], 0)
    offset = lax.broadcasted_iota(jnp.int32, (rows, entries), 0) * columns + me - start
    begin = place * columns
    arrive = jnp.where((offset >= begin) & (offset < begin + columns) & (offset < length),
                       1.0, 0.0).astype(F32)

    cells = jnp.concatenate(
        [phi_ref[2 * pair + k, y] for pair in range(edge // 2) for y in range(edge) for k in range(2)],
        axis=0)
    leave[...] = dot(placing, cells, ((1,), (1,))).reshape(leave.shape)

    held = (lax.broadcasted_iota(jnp.int32, (rows, tiles), 0) * columns + me
            == lax.broadcasted_iota(jnp.int32, (rows, tiles), 1))

    def link(face):
        there = jnp.where(links_ref[face] >= 0, 1.0, 0.0).astype(F32)
        value = jnp.sum(jnp.where(held, there, 0.0), axis=1, keepdims=True)
        return jnp.broadcast_to(value, (rows, LANES))

    link_x = [link(0), link(1)]
    link_y = link(2)
    link_z = [link(4), link(5)]
    lane = lax.broadcasted_iota(jnp.int32, (rows, LANES), 1)
    z = lane % wide

    pl.semaphore_wait(barrier, columns - 1 + has_below.astype(jnp.int32) + has_above.astype(jnp.int32))
    sent = exchange(leave, land, out_send, out_recv)

    packed = dot(arrive, land[...].reshape(-1, land.shape[2]), ((1,), (0,)))
    mine = []
    for pair in range(edge // 2):
        both = packed[:, pair * LANES:(pair + 1) * LANES]
        mine += [roll(both, halo, 1), roll(both, halo - edge, 1)]

    parts = mine + [link_y] + link_x
    slots = up.shape[0]
    for q in range(slots):
        high, low = jnp.zeros((rows, LANES), F32), jnp.zeros((rows, LANES), F32)
        for k in range(4):
            if 4 * q + k < len(parts):
                inside = (z >= halo * k) & (z < halo * (k + 1))
                part = parts[4 * q + k]
                high = jnp.where(inside, roll(part, halo * k - edge, 1), high)
                low = jnp.where(inside, roll(part, halo * k - halo, 1), low)
        up[q] = high
        down[q] = low
    both_ways("grp", grp, has_above, has_below, up, down, from_below, from_above, 0)()

    filled = []
    for i, part in enumerate(parts):
        q, k = divmod(i, 4)
        below = roll(from_below[q], -halo * k, 1)
        above = roll(from_above[q], halo + edge - halo * k, 1)
        filled.append(jnp.where(z < halo, below, jnp.where(z >= halo + edge, above, part)))
    mine, link_y, link_x = filled[:edge], filled[edge], filled[edge + 1:]
    link_z = jnp.where(z == halo, link_z[0], jnp.where(z == halo + edge, link_z[1],
                       jnp.where(z == 0, 0.0, 1.0)))
    link_y = jnp.where(lane < wide, link_y, 1.0)

    for k in range(halo):
        right[k] = mine[edge - halo + k]
        left[k] = mine[k]
    for ref in (right, left):
        ref[halo] = link_y
        ref[halo + 1] = link_z
    arrived = both_ways("mem", me, has_right, has_left, right, left, from_left, from_right, 2)

    masks_y, masks_z = [None, link_y, None], [None, link_z, None]

    def begin_layer(i, value):
        level[0, i] = value
        sign[i] = value / jnp.sqrt(value * value + 1.0)

    def sweep(step, low, high):
        now, later = step % 2, (step + 1) % 2
        gap = None
        for i in range(low, high):
            region = 0 if i < halo else (1 if i < halo + edge else 2)
            mask_y, mask_z = masks_y[region], masks_z[region]
            value, field = level[now, i], sign[i]
            side = jnp.where(field > 0, 1.0, -1.0)

            def across(j):
                change = level[now, j] - level[now, j - 1]
                if j == halo:
                    change = change * link_x[0]
                elif j == halo + edge:
                    change = change * link_x[1]
                return change

            gap = across(i) if gap is None else gap
            ahead = across(i + 1)
            most = jnp.maximum(jnp.maximum(side * gap, -(side * ahead)), 0.0)
            squares = most * most
            gap = ahead

            turned = roll(value, wide, 1)
            before = jnp.where(lane < wide, roll(turned, 1, 0), turned)
            behind = (value - before) * mask_y
            turned = roll(behind, -wide, 1)
            ahead = jnp.where(lane >= LANES - wide, roll(turned, -1, 0), turned)
            most = jnp.maximum(jnp.maximum(side * behind, -(side * ahead)), 0.0)
            squares = squares + most * most

            behind = (value - roll(value, 1, 1)) * mask_z
            ahead = roll(behind, -1, 1)
            most = jnp.maximum(jnp.maximum(side * behind, -(side * ahead)), 0.0)
            squares = squares + most * most
            level[later, i] = value - TIME_STEP * field * (jnp.sqrt(squares + EPSILON) - 1.0)

    for i in range(edge):
        begin_layer(halo + i, mine[i])
    sweep(0, halo + 1, halo + edge - 1)
    arrived()
    masks_y[0], masks_y[2] = from_left[halo], from_right[halo]
    masks_z[0], masks_z[2] = from_left[halo + 1], from_right[halo + 1]
    for i in range(halo):
        begin_layer(i, from_left[i])
        begin_layer(halo + edge + i, from_right[i])
    sweep(0, 1, halo + 1)
    sweep(0, halo + edge - 1, layers - 1)
    for step in range(1, STEPS):
        sweep(step, step + 1, layers - 1 - step)

    last = STEPS % 2
    pairs = []
    for pair in range(edge // 2):
        first, second = level[last, halo + 2 * pair], level[last, halo + 2 * pair + 1]
        pairs.append(jnp.where(z < edge, roll(first, -halo, 1), roll(second, edge - halo, 1)))
    final = jnp.concatenate(pairs, axis=1)
    back[...] = dot(arrive, final, ((0,), (0,))).reshape(back.shape)
    sent += exchange(back, home, back_send, back_recv)

    living = jnp.where(slot < count, placing, 0.0)
    owned = dot(living, home[...].reshape(-1, home.shape[2]), ((0,), (0,))).T
    for pair in range(edge // 2):
        for y in range(edge):
            for k in range(2):
                at = ((pair * edge + y) * 2 + k) * edge
                out_ref[2 * pair + k, y] = owned[at:at + edge]
    for copy in sent:
        copy.wait_send()
    for there, copy in late:
        pl.when(there)(copy.wait_send)


def on_device(phi_owned, band_counts, neighbours):
    edge, own_slots = phi_owned.shape[0], phi_owned.shape[3]
    columns, groups = lax.axis_size("mem"), lax.axis_size("grp")
    rows = neighbours.shape[2] // columns
    padded = -(-own_slots // (8 * columns)) * 8
    halo, cells = STEPS, edge * edge * edge
    vmem = pl.BlockSpec(memory_space=pltpu.VMEM)
    buffer = pltpu.VMEM((columns, padded, cells), F32)
    strip = pltpu.VMEM((-(-(edge + 3) // 4), rows, LANES), F32)
    face = pltpu.VMEM((halo + 2, rows, LANES), F32)
    layers = edge + 2 * halo
    return pl.pallas_call(
        functools.partial(kernel, columns, groups),
        out_shape=jax.ShapeDtypeStruct(phi_owned.shape, F32),
        in_specs=[vmem, pl.BlockSpec(memory_space=pltpu.SMEM), vmem],
        out_specs=vmem,
        scratch_shapes=[buffer] * 4 + [strip] * 4 + [face] * 4 + [
            pltpu.VMEM((2, layers, rows, LANES), F32),
            pltpu.VMEM((layers, rows, LANES), F32),
        ] + [pltpu.SemaphoreType.DMA((columns,))] * 4 + [pltpu.SemaphoreType.DMA((4,))] * 2,
        compiler_params=pltpu.CompilerParams(collective_id=0, has_side_effects=True),
    )(phi_owned, band_counts, jnp.transpose(neighbours, (1, 0, 2)))


def solution(mesh):
    return jax.shard_map(
        on_device,
        mesh=mesh,
        in_specs=(P(None, None, None, ("grp", "mem")), P("grp", None), P("grp", None, None)),
        out_specs=P(None, None, None, ("grp", "mem")),
        check_vma=False,
    )
```
